32 devices in a mesh: row: 16 (over z, y, x), col: 2 (over core).
Axes of the slice: x: 2, y: 2, z: 4, core: 2. Of those that a mesh axis runs over, the one named last changes fastest.
Arguments:
- incident: bfloat16 [2, 8192, 512], P(None, ('row', 'col')), may hold values from -6 to 6
- near_tiles: bfloat16 [32, 2, 3, 2, 256, 256], P(('row', 'col')), may hold values from -0.15625 to 0.15625
- near_offsets: int32 [32, 3], P(('row', 'col')), may hold values from -2 to 2, as said below
- far_row: int32 [16, 2, 16], P('row', 'col'), may hold values from 0 to 1, as said below
- far_col: int32 [16, 2, 16], P('row', 'col'), may hold values from 0 to 15
- far_rank: int32 [16, 2, 16], P('row', 'col'), may hold values from 8 to 32, as said below
- far_count: int32 [16, 2], P('row', 'col'), may hold values from 2 to 16, as said below
- far_u: bfloat16 [16, 2, 2, 16, 2, 32, 256], P('row', 'col'), may hold values from -0.25 to 0.25
- far_v: bfloat16 [16, 2, 2, 16, 2, 32, 256], P('row', 'col'), may hold values from -0.25 to 0.25
Outputs:
- response: bfloat16 [2, 8192, 512], P(None, ('row', 'col'))
The draws below stay inside these ranges and needn't reach their ends.
Inputs may be any that keep to these rules, and one draw needn't show every extreme that they name: `near_offsets`: slot 0 of every tile is 0; the other slots of a tile hold distinct values among -2, -1, 1, 2. On one device the pairs (far_row, far_col) of all 16 slots are distinct, and every block (i, j) they name has circular tile distance 3 or more between i and j. `far_rank`: slot 0 of every device has rank 32. `far_count`: some device has all 16 slots live.
All inputs are finite; a program needn't handle non-finite values.
Results may differ from the reference program's by a relative error of at most 0.0035.
Values may be sent and summed in bfloat16 or wider, within the bound.
No kernel may reach another device: no remote copies, remote signals or barrier semaphores. Data moves between devices by JAX's collectives and lax.ppermute only.
A program may use at most 192 MiB of HBM per device.

```python
import jax
import jax.numpy as jnp
from jax import lax

TILE = 256
RANK = 32
NEAR_SLOTS = 3
WAVES = 2
SOURCES = 256
FAR_SLOTS = 16
TILES = 32
PANELS = 8192
N_ROW = 16
N_COL = 2


def draw_near_offsets(key, part):
    tile_count = N_ROW * N_COL
    scores = jax.random.randint(jax.random.fold_in(key, 11), (tile_count, 4), 0, 1 << 20) * 4 + jnp.arange(4, dtype=jnp.int32)[None, :]
    ranking = jnp.argsort(scores, axis=1)
    offset_table = jnp.array([-2, -1, 1, 2], dtype=jnp.int32)
    picked = offset_table[ranking[:, :NEAR_SLOTS - 1]]
    return jnp.concatenate([jnp.zeros((tile_count, 1), jnp.int32), picked], axis=1).astype(jnp.int32)


def far_layout(key):
    pair_count = N_COL * N_ROW
    tile_count = N_ROW * N_COL
    pair_ids = jnp.arange(pair_count, dtype=jnp.int32)
    local_row = pair_ids // N_ROW
    col_device = pair_ids % N_ROW
    row_index = jnp.arange(N_ROW, dtype=jnp.int32)[:, None, None]
    col_index = jnp.arange(N_COL, dtype=jnp.int32)[None, :, None]
    row_tile = row_index * N_COL + local_row[None, None, :]
    col_tile = col_device[None, None, :] * N_COL + col_index
    forward_gap = (row_tile - col_tile) % tile_count
    circular = jnp.minimum(forward_gap, tile_count - forward_gap)
    random_part = jax.random.randint(jax.random.fold_in(key, 21), (N_ROW, N_COL, pair_count), 0, 1 << 19)
    scores = random_part * 1024 + pair_ids[None, None, :] + jnp.where(circular < 3, 1 << 30, 0)
    ranking = jnp.argsort(scores, axis=2)[:, :, :FAR_SLOTS]
    return ((ranking // N_ROW).astype(jnp.int32), (ranking % N_ROW).astype(jnp.int32))


def draw_far_row(key, part):
    return far_layout(key)[0]


def draw_far_col(key, part):
    return far_layout(key)[1]


def draw_far_rank(key, part):
    sampled = jax.random.randint(jax.random.fold_in(key, 31), (N_ROW, N_COL, FAR_SLOTS), max(1, RANK // 4), RANK + 1)
    leading = (jnp.arange(FAR_SLOTS, dtype=jnp.int32) == 0)[None, None, :]
    return jnp.where(leading, RANK, sampled).astype(jnp.int32)


def draw_far_count(key, part):
    lowest = max(1, FAR_SLOTS // 8)
    spread = FAR_SLOTS - lowest
    uniform_part = jax.random.randint(jax.random.fold_in(key, 41), (N_ROW, N_COL), 0, spread + 1)
    counts = lowest + uniform_part * uniform_part // spread
    fullest = jax.random.randint(jax.random.fold_in(key, 42), (), 0, N_ROW * N_COL)
    flat_index = jnp.arange(N_ROW * N_COL, dtype=jnp.int32).reshape(N_ROW, N_COL)
    return jnp.where(flat_index == fullest, FAR_SLOTS, counts).astype(jnp.int32)


def levels(rng, extent, pieces, least, high):
    def one(position, parts):
        draws = jax.random.uniform(jax.random.fold_in(jax.random.fold_in(rng, 6), position), (parts,), jnp.float32, least / len(pieces), high / len(pieces))
        return jnp.repeat(jnp.exp(draws), extent[position] // parts).reshape((-1,) + (1,) * (len(extent) - position - 1))

    loudness = one(*pieces[0])
    for cut in pieces[1:]:
        loudness = loudness * one(*cut)
    return loudness


def normal_values(own_key, extent, width, most, pieces=(), held_as=jnp.bfloat16):
    level = levels(own_key, extent, pieces, -0.22, 0.18) if pieces else 1.0
    drawn = jax.random.normal(own_key, extent, jnp.float32) * width * level
    return jnp.minimum(jnp.maximum(drawn, -most), most).astype(held_as)


def setup_inputs(seed: int = 0) -> dict:
    keys = jax.random.split(jax.random.key(seed), 10)
    return {
        "incident": normal_values(keys[0], (WAVES, PANELS, 2 * SOURCES), 1.0, 6.0, ((1, 32),)),
        "near_tiles": normal_values(keys[1], (TILES, WAVES, NEAR_SLOTS, 2, TILE, TILE), (2 * TILE * NEAR_SLOTS) ** -0.5, 0.15625, ((0, 32),)),
        "near_offsets": draw_near_offsets(jax.random.fold_in(keys[9], 71), 0),
        "far_row": draw_far_row(jax.random.fold_in(keys[9], 71), 0),
        "far_col": draw_far_col(jax.random.fold_in(keys[9], 71), 0),
        "far_rank": draw_far_rank(jax.random.fold_in(keys[9], 71), 0),
        "far_count": draw_far_count(jax.random.fold_in(keys[9], 71), 0),
        "far_u": normal_values(keys[7], (N_ROW, N_COL, WAVES, FAR_SLOTS, 2, RANK, TILE), (RANK * FAR_SLOTS) ** -0.5, 0.25, ((0, 16), (1, 2))),
        "far_v": normal_values(keys[8], (N_ROW, N_COL, WAVES, FAR_SLOTS, 2, RANK, TILE), (2 * TILE) ** -0.5, 0.25, ((0, 16), (1, 2))),
    }


def combine_parts(real_prod, imag_prod):
    half_width = real_prod.shape[-1] // 2
    return jnp.concatenate([real_prod[..., :half_width] - imag_prod[..., half_width:], real_prod[..., half_width:] + imag_prod[..., :half_width]], axis=-1)


def reference(incident, near_tiles, near_offsets, far_row, far_col, far_rank, far_count, far_u, far_v):
    tile_count = N_ROW * N_COL
    columns = incident.shape[-1]
    tiles_input = incident.reshape(WAVES, tile_count, TILE, columns)
    near_groups = near_tiles.reshape(N_ROW, N_COL, WAVES, NEAR_SLOTS, 2, TILE, TILE)
    offset_groups = near_offsets.reshape(N_ROW, N_COL, NEAR_SLOTS)
    slot_ids = jnp.arange(FAR_SLOTS, dtype=jnp.int32)
    rank_ids = jnp.arange(RANK, dtype=jnp.int32)
    block_ids = jnp.arange(N_COL, dtype=jnp.int32)

    def one_group(packed):
        group_index, near_part, offset_part, rows_part, cols_part, rank_part, count_part, u_part, v_part = packed
        own_tiles = group_index * N_COL + block_ids
        near_index = ((own_tiles[:, None] + offset_part) % tile_count).astype(jnp.int32)
        near_inputs = tiles_input[:, near_index].astype(jnp.float32)
        near_float = near_part.astype(jnp.float32)
        real_prod = jnp.einsum("awnpq,wanqc->wapc", near_float[:, :, :, 0], near_inputs)
        imag_prod = jnp.einsum("awnpq,wanqc->wapc", near_float[:, :, :, 1], near_inputs)
        result_rows = combine_parts(real_prod, imag_prod)
        for col_group in range(N_COL):
            col_tiles = (cols_part[col_group] * N_COL + col_group).astype(jnp.int32)
            live_mask = ((slot_ids < count_part[col_group])[:, None] & (rank_ids[None, :] < rank_part[col_group][:, None])).astype(jnp.float32)
            select = (rows_part[col_group][:, None] == block_ids[None, :]).astype(jnp.float32)
            for wave_index in range(WAVES):
                slot_tiles = tiles_input[wave_index, col_tiles].astype(jnp.float32)
                v_factor = v_part[col_group, wave_index].astype(jnp.float32)
                coefficients = combine_parts(jnp.einsum("fkq,fqc->fkc", v_factor[:, 0], slot_tiles), jnp.einsum("fkq,fqc->fkc", v_factor[:, 1], slot_tiles))
                coefficients = lax.optimization_barrier((coefficients * live_mask[:, :, None]).astype(jnp.bfloat16)).astype(jnp.float32)
                u_factor = u_part[col_group, wave_index].astype(jnp.float32)
                contrib = combine_parts(jnp.einsum("fkp,fkc->fpc", u_factor[:, 0], coefficients), jnp.einsum("fkp,fkc->fpc", u_factor[:, 1], coefficients))
                added = jnp.einsum("fa,fpc->apc", select, contrib, precision=lax.Precision.HIGHEST)
                result_rows = result_rows.at[wave_index].add(added)
        return result_rows.astype(jnp.bfloat16)

    grouped = lax.map(one_group, (jnp.arange(N_ROW, dtype=jnp.int32), near_groups, offset_groups, far_row, far_col, far_rank, far_count, far_u, far_v))
    return jnp.transpose(grouped, (1, 0, 2, 3, 4)).reshape(WAVES, tile_count * TILE, columns)
```

```python
import functools

import jax
import jax.numpy as jnp
from jax import lax
from jax.experimental import pallas as pl
from jax.experimental.pallas import tpu as pltpu
from jax.sharding import PartitionSpec as P


def ring_sizes(count):
    last = 2 if count % 2 == 0 else 1
    rest = count // last
    lead = 4 if rest % 4 == 0 else rest
    return (lead, rest // lead, last)


def split_row(row, sizes):
    return (row // (sizes[1] * sizes[2]), (row // sizes[2]) % sizes[1], row % sizes[2])


def join_row(parts, sizes):
    return (parts[0] * sizes[1] + parts[1]) * sizes[2] + parts[2]


def shifted_row(row, offset, sizes):
    parts = split_row(row, sizes)
    return join_row(tuple((p + o) % n for p, o, n in zip(parts, offset, sizes)), sizes)


def fetch(value, offset, sizes):
    count = sizes[0] * sizes[1] * sizes[2]
    pairs = [(shifted_row(row, offset, sizes), row) for row in range(count)]
    return lax.ppermute(value, "row", pairs)


def gather_wave(own, order, sizes):
    pieces = {(0, 0, 0): own}
    for axis in order:
        for offset, value in list(pieces.items()):
            for step in range(1, sizes[axis]):
                jump = tuple(step if k == axis else 0 for k in range(3))
                reached = tuple(step if k == axis else o for k, o in enumerate(offset))
                pieces[reached] = fetch(value, jump, sizes)
    return pieces


def pick_row(pieces, move, row, sizes):
    count = sizes[0] * sizes[1] * sizes[2]
    groups = {}
    for own in range(count):
        there = split_row((own + move) % count, sizes)
        here = split_row(own, sizes)
        offset = tuple((t - h) % n for t, h, n in zip(there, here, sizes))
        groups.setdefault(offset, []).append(own)
    chosen = None
    for offset, members in sorted(groups.items()):
        if chosen is None:
            chosen = pieces[offset]
        else:
            inside = functools.reduce(jnp.logical_or, [row == member for member in members])
            chosen = jnp.where(inside, pieces[offset], chosen)
    return chosen


def mixed(real, imag):
    half = real.shape[-1] // 2
    return jnp.concatenate(
        [real[:, :half] - imag[:, half:], real[:, half:] + imag[:, :half]], axis=-1
    )


def wave_kernel(slot_ref, rank_ref, near_ref, turn_ref, v_ref, u_ref, tiles_ref, *rest, count, blocks):
    pieces = rest[:count]
    around = rest[count : count + 4]
    others_ref, mine_ref, coef_ref, factor_ref, around_ref = rest[count + 4 :]
    rank_size, tile = v_ref.shape[2], v_ref.shape[3]
    columns = coef_ref.shape[2]
    rank_ids = lax.broadcasted_iota(jnp.int32, (rank_size, columns), 0)
    for m in range(count):
        factors = jnp.concatenate(
            [v_ref[slot_ref[a * count + m]].reshape(2 * rank_size, tile) for a in range(blocks)], axis=0
        )
        prod = jnp.dot(factors, pieces[m][...], preferred_element_type=jnp.float32)
        for a in range(blocks):
            low = 2 * a * rank_size
            value = mixed(prod[low : low + rank_size], prod[low + rank_size : low + 2 * rank_size])
            value = jnp.where(rank_ids < rank_ref[a * count + m], value, 0.0)
            coef_ref[a, m * rank_size : (m + 1) * rank_size, :] = value.astype(jnp.bfloat16)

    def block_sum(a):
        for m in range(count):
            slot = slot_ref[a * count + m]
            for part in range(2):
                factor_ref[part, m * rank_size : (m + 1) * rank_size, :] = u_ref[slot, part]
        coef = coef_ref[a]
        dims = (((0,), (0,)), ((), ()))
        real = lax.dot_general(factor_ref[0], coef, dims, preferred_element_type=jnp.float32)
        imag = lax.dot_general(factor_ref[1], coef, dims, preferred_element_type=jnp.float32)
        return mixed(real, imag)

    for step in range(1, blocks):
        others_ref[step - 1] = block_sum(lax.rem(turn_ref[0] + step, blocks)).astype(jnp.bfloat16)
    total = block_sum(turn_ref[0])
    around_ref[2] = pieces[0][...]
    for k, place in enumerate((0, 1, 3, 4)):
        around_ref[place] = around[k][...]
    prod = None
    for n in range(tiles_ref.shape[0]):
        matrix = tiles_ref[n].reshape(2 * tile, tile)
        term = jnp.dot(matrix, around_ref[near_ref[n] + 2], preferred_element_type=jnp.float32)
        prod = term if prod is None else prod + term
    mine_ref[...] = total + mixed(prod[:tile], prod[tile:])


def wave_sums(slots, ranks, offsets, turn, v_wave, u_wave, tiles, pieces, around, blocks):
    count = len(pieces)
    tile, columns = pieces[0].shape
    rank_size = v_wave.shape[2]
    smem = pl.BlockSpec(memory_space=pltpu.SMEM)
    vmem = pl.BlockSpec(memory_space=pltpu.VMEM)
    flops = 2 * tile * columns * (4 * blocks * count * rank_size + 2 * tiles.shape[0] * tile)
    return pl.pallas_call(
        functools.partial(wave_kernel, count=count, blocks=blocks),
        out_shape=(
            jax.ShapeDtypeStruct((blocks - 1, tile, columns), jnp.bfloat16),
            jax.ShapeDtypeStruct((tile, columns), jnp.float32),
        ),
        in_specs=[smem] * 4 + [vmem] * (3 + count + 4),
        out_specs=(vmem, vmem),
        scratch_shapes=[
            pltpu.VMEM((blocks, count * rank_size, columns), jnp.bfloat16),
            pltpu.VMEM((2, count * rank_size, tile), jnp.bfloat16),
            pltpu.VMEM((5, tile, columns), jnp.bfloat16),
        ],
        cost_estimate=pl.CostEstimate(
            flops=flops, bytes_accessed=2 * count * tile * columns, transcendentals=0
        ),
    )(slots, ranks, offsets, turn, v_wave, u_wave, tiles, *pieces, *around)


def shards(incident, near_tiles, near_offsets, far_row, far_col, far_rank, far_count, far_u, far_v):
    wave_count = incident.shape[0]
    rows, blocks = lax.axis_size("row"), lax.axis_size("col")
    sizes = ring_sizes(rows)
    row, col = lax.axis_index("row"), lax.axis_index("col")

    orders = ((0, 1, 2), (0, 2, 1))
    waves = [
        gather_wave(incident[w], orders[w % 2], sizes) for w in range(wave_count)
    ]
    keys = sorted(waves[0])

    sources = jnp.stack([shifted_row(row, key, sizes) for key in keys]).astype(jnp.int32)
    slot_ids = jnp.arange(far_row.shape[2], dtype=jnp.int32)
    match = (
        (far_row[0, 0][None, None, :] == jnp.arange(blocks, dtype=jnp.int32)[:, None, None])
        & (far_col[0, 0][None, None, :] == sources[None, :, None])
        & (slot_ids < far_count[0, 0])[None, None, :]
    )
    slots = jnp.sum(jnp.where(match, slot_ids, 0), axis=2).reshape(-1).astype(jnp.int32)
    ranks = jnp.sum(jnp.where(match, far_rank[0, 0], 0), axis=2).reshape(-1).astype(jnp.int32)
    turn = col.reshape(1).astype(jnp.int32)

    def flat_fetch(value, move):
        total = rows * blocks
        pairs = [((d + move) % total, d) for d in range(total)]
        return lax.ppermute(value, ("row", "col"), pairs)

    results = []
    for w in range(wave_count):
        pieces, own = waves[w], incident[w]
        if blocks == 2:
            swap = [(0, 1), (1, 0)]
            before, after = pick_row(pieces, -1, row, sizes), pick_row(pieces, 1, row, sizes)
            beside = lax.ppermute(own, "col", swap)
            beyond = lax.ppermute(jnp.where(col == 0, after, before), "col", swap)
            around = (
                before,
                jnp.where(col == 0, beyond, beside),
                jnp.where(col == 0, beside, beyond),
                after,
            )
        else:
            around = tuple(flat_fetch(own, move) for move in (-2, -1, 1, 2))
        others, mine = wave_sums(
            slots, ranks, near_offsets[0], turn, far_v[0, 0, w], far_u[0, 0, w], near_tiles[0, w],
            [pieces[key] for key in keys], around, blocks,
        )
        for step in range(1, blocks):
            pairs = [(c, (c + step) % blocks) for c in range(blocks)]
            mine = mine + lax.ppermute(others[step - 1], "col", pairs).astype(jnp.float32)
        results.append(mine.astype(jnp.bfloat16))
    return jnp.stack(results, axis=0)


def solution(mesh):
    in_specs = (
        P(None, ("row", "col"), None),
        P(("row", "col"), None, None, None, None, None),
        P(("row", "col"), None),
        P("row", "col", None),
        P("row", "col", None),
        P("row", "col", None),
        P("row", "col"),
        P("row", "col", None, None, None, None, None),
        P("row", "col", None, None, None, None, None),
    )
    out_specs = P(None, ("row", "col"), None)
    return jax.shard_map(shards, mesh=mesh, in_specs=in_specs, out_specs=out_specs, check_vma=False)
```

```python
import functools

import jax
import jax.numpy as jnp
from jax import lax
from jax.experimental import pallas as pl
from jax.experimental.pallas import tpu as pltpu
from jax.sharding import PartitionSpec as P


def fetch(value, flip, count):
    return lax.ppermute(value, "row", [(row ^ flip, row) for row in range(count)])


def gather_wave(own, order, count):
    pieces = {0: own}
    for bit in order:
        for offset, value in list(pieces.items()):
            pieces[offset ^ (1 << bit)] = fetch(value, 1 << bit, count)
    return pieces


def pick_row(pieces, move, row):
    count = len(pieces)
    groups = {}
    for own in range(count):
        groups.setdefault(own ^ ((own + move) % count), []).append(own)
    chosen = None
    for offset, members in sorted(groups.items()):
        if chosen is None:
            chosen = pieces[offset]
        else:
            inside = functools.reduce(jnp.logical_or, [row == member for member in members])
            chosen = jnp.where(inside, pieces[offset], chosen)
    return chosen


def mixed(real, imag):
    half = real.shape[-1] // 2
    return jnp.concatenate(
        [real[:, :half] - imag[:, half:], real[:, half:] + imag[:, :half]], axis=-1
    )


def wave_kernel(slot_ref, rank_ref, near_ref, turn_ref, v_ref, u_ref, tiles_ref, *rest, count, blocks):
    pieces = rest[:count]
    around = rest[count : count + 4]
    others_ref, mine_ref, coef_ref, factor_ref, around_ref = rest[count + 4 :]
    rank_size, tile = v_ref.shape[2], v_ref.shape[3]
    columns = coef_ref.shape[2]
    rank_ids = lax.broadcasted_iota(jnp.int32, (rank_size, columns), 0)
    for m in range(count):
        factors = jnp.concatenate(
            [v_ref[slot_ref[a * count + m]].reshape(2 * rank_size, tile) for a in range(blocks)], axis=0
        )
        prod = jnp.dot(factors, pieces[m][...], preferred_element_type=jnp.float32)
        for a in range(blocks):
            low = 2 * a * rank_size
            value = mixed(prod[low : low + rank_size], prod[low + rank_size : low + 2 * rank_size])
            value = jnp.where(rank_ids < rank_ref[a * count + m], value, 0.0)
            coef_ref[a, m * rank_size : (m + 1) * rank_size, :] = value.astype(jnp.bfloat16)

    def block_sum(a):
        for m in range(count):
            slot = slot_ref[a * count + m]
            for part in range(2):
                factor_ref[part, m * rank_size : (m + 1) * rank_size, :] = u_ref[slot, part]
        coef = coef_ref[a]
        dims = (((0,), (0,)), ((), ()))
        real = lax.dot_general(factor_ref[0], coef, dims, preferred_element_type=jnp.float32)
        imag = lax.dot_general(factor_ref[1], coef, dims, preferred_element_type=jnp.float32)
        return mixed(real, imag)

    for step in range(1, blocks):
        others_ref[step - 1] = block_sum(lax.rem(turn_ref[0] + step, blocks)).astype(jnp.bfloat16)
    total = block_sum(turn_ref[0])
    around_ref[2] = pieces[0][...]
    for k, place in enumerate((0, 1, 3, 4)):
        around_ref[place] = around[k][...]
    prod = None
    for n in range(tiles_ref.shape[0]):
        matrix = tiles_ref[n].reshape(2 * tile, tile)
        term = jnp.dot(matrix, around_ref[near_ref[n] + 2], preferred_element_type=jnp.float32)
        prod = term if prod is None else prod + term
    mine_ref[...] = total + mixed(prod[:tile], prod[tile:])


def wave_sums(slots, ranks, offsets, turn, v_wave, u_wave, tiles, pieces, around, blocks):
    count = len(pieces)
    tile, columns = pieces[0].shape
    rank_size = v_wave.shape[2]
    smem = pl.BlockSpec(memory_space=pltpu.SMEM)
    vmem = pl.BlockSpec(memory_space=pltpu.VMEM)
    flops = 2 * tile * columns * (4 * blocks * count * rank_size + 2 * tiles.shape[0] * tile)
    return pl.pallas_call(
        functools.partial(wave_kernel, count=count, blocks=blocks),
        out_shape=(
            jax.ShapeDtypeStruct((blocks - 1, tile, columns), jnp.bfloat16),
            jax.ShapeDtypeStruct((tile, columns), jnp.float32),
        ),
        in_specs=[smem] * 4 + [vmem] * (3 + count + 4),
        out_specs=(vmem, vmem),
        scratch_shapes=[
            pltpu.VMEM((blocks, count * rank_size, columns), jnp.bfloat16),
            pltpu.VMEM((2, count * rank_size, tile), jnp.bfloat16),
            pltpu.VMEM((5, tile, columns), jnp.bfloat16),
        ],
        cost_estimate=pl.CostEstimate(
            flops=flops, bytes_accessed=2 * count * tile * columns, transcendentals=0
        ),
    )(slots, ranks, offsets, turn, v_wave, u_wave, tiles, *pieces, *around)


def shards(incident, near_tiles, near_offsets, far_row, far_col, far_rank, far_count, far_u, far_v):
    wave_count = incident.shape[0]
    rows, blocks = lax.axis_size("row"), lax.axis_size("col")
    row, col = lax.axis_index("row"), lax.axis_index("col")

    top = rows.bit_length() - 2
    middle = tuple(range(top - 1, 1, -1))
    orders = ((top, 1) + middle + (0,), (top, 0) + middle + (1,))
    waves = [gather_wave(incident[w], orders[w % 2], rows) for w in range(wave_count)]
    keys = sorted(waves[0])

    sources = jnp.stack([row ^ key for key in keys]).astype(jnp.int32)
    slot_ids = jnp.arange(far_row.shape[2], dtype=jnp.int32)
    match = (
        (far_row[0, 0][None, None, :] == jnp.arange(blocks, dtype=jnp.int32)[:, None, None])
        & (far_col[0, 0][None, None, :] == sources[None, :, None])
        & (slot_ids < far_count[0, 0])[None, None, :]
    )
    slots = jnp.sum(jnp.where(match, slot_ids, 0), axis=2).reshape(-1).astype(jnp.int32)
    ranks = jnp.sum(jnp.where(match, far_rank[0, 0], 0), axis=2).reshape(-1).astype(jnp.int32)
    turn = col.reshape(1).astype(jnp.int32)

    def flat_fetch(value, move):
        total = rows * blocks
        pairs = [((d + move) % total, d) for d in range(total)]
        return lax.ppermute(value, ("row", "col"), pairs)

    results = []
    for w in range(wave_count):
        pieces, own = waves[w], incident[w]
        if blocks == 2:
            swap = [(0, 1), (1, 0)]
            before, after = pick_row(pieces, -1, row), pick_row(pieces, 1, row)
            beside = lax.ppermute(own, "col", swap)
            beyond = lax.ppermute(jnp.where(col == 0, after, before), "col", swap)
            around = (
                before,
                jnp.where(col == 0, beyond, beside),
                jnp.where(col == 0, beside, beyond),
                after,
            )
        else:
            around = tuple(flat_fetch(own, move) for move in (-2, -1, 1, 2))
        others, mine = wave_sums(
            slots, ranks, near_offsets[0], turn, far_v[0, 0, w], far_u[0, 0, w], near_tiles[0, w],
            [pieces[key] for key in keys], around, blocks,
        )
        for step in range(1, blocks):
            pairs = [(c, (c + step) % blocks) for c in range(blocks)]
            mine = mine + lax.ppermute(others[step - 1], "col", pairs).astype(jnp.float32)
        results.append(mine.astype(jnp.bfloat16))
    return jnp.stack(results, axis=0)


def solution(mesh):
    in_specs = (
        P(None, ("row", "col"), None),
        P(("row", "col"), None, None, None, None, None),
        P(("row", "col"), None),
        P("row", "col", None),
        P("row", "col", None),
        P("row", "col", None),
        P("row", "col"),
        P("row", "col", None, None, None, None, None),
        P("row", "col", None, None, None, None, None),
    )
    out_specs = P(None, ("row", "col"), None)
    return jax.shard_map(shards, mesh=mesh, in_specs=in_specs, out_specs=out_specs, check_vma=False)
```
